128 devices in a mesh: blk: 32 (over z, x, core), col: 4 (over y).
Axes of the slice: x: 4, y: 4, z: 4, core: 2. Of those that a mesh axis runs over, the one named last changes fastest.
Arguments:
- pixel_row: int32 [32768, 256], P(('blk', 'col')), may hold values from 0 to 63, as said below
- pixel_col: int32 [32768, 256], P(('blk', 'col')), may hold values from 0 to 2047, as said below
- strip_of_span: int32 [128, 256], P(('blk', 'col')), may hold values from 0 to 127, as said below
- shear_one: float32 [32768, 256], P(('blk', 'col')), may hold values from -6 to 6
- shear_two: float32 [32768, 256], P(('blk', 'col')), may hold values from -6 to 6
- weight: float32 [32768, 256], P(('blk', 'col')), may hold values from 0.25 to 4
Outputs:
- kappa_e: float32 [8192, 8192], P(('blk', 'col'))
- kappa_b: float32 [8192, 8192], P(('blk', 'col'))
The draws below stay inside these ranges and needn't reach their ends.
Inputs may be any that keep to these rules, and one draw needn't show every extreme that they name: `pixel_row`: all galaxies of one span (one row) lie in one aligned band of 8 rows. `pixel_col`: all galaxies of one span (one row) lie in one aligned block of 128 columns. `strip_of_span`: row d names the row strip of each span of shard d; each strip is named exactly 2 times in every row.
All inputs are finite; a program needn't handle non-finite values.
Results may differ from the reference program's by a relative error of at most 0.0038.
Values may be sent and summed in bfloat16 or wider, within the bound.
No kernel may reach another device: no remote copies, remote signals or barrier semaphores. Data moves between devices by JAX's collectives and lax.ppermute only.
A program may use at most 128 MiB of HBM per device.

```python
import math
import jax
import jax.numpy as jnp
from jax import lax

SLAB = 256
TILE_COLS = 2048
BAND = 8
SUBC = 128
GAL = 256
DEPTH = 2
STRIP = 64
SHARD_SPANS = 256
SPANS = 32768
N_BLK = 32
N_COL = 4


def draw_pixel_row(key, part):
    band_key, offset_key = jax.random.split(jax.random.fold_in(key, 11))
    band_pick = jax.random.randint(band_key, (SPANS, 1), 0, STRIP // BAND)
    offsets = jax.random.randint(offset_key, (SPANS, GAL), 0, BAND)
    return (band_pick * BAND + offsets).astype(jnp.int32)


def draw_pixel_col(key, part):
    block_key, offset_key = jax.random.split(jax.random.fold_in(key, 23))
    blocks = jax.random.randint(block_key, (SPANS, 1), 0, TILE_COLS // SUBC)
    offsets = jax.random.randint(offset_key, (SPANS, GAL), 0, SUBC)
    return (blocks * SUBC + offsets).astype(jnp.int32)


def draw_strip_of_span(key, part):
    row_keys = jax.random.split(jax.random.fold_in(key, 31), N_BLK * N_COL)
    orders = jax.vmap(lambda one_key: jax.random.permutation(one_key, SHARD_SPANS))(row_keys)
    return (orders % (SHARD_SPANS // DEPTH)).astype(jnp.int32)


def block_levels(own_key, dims, pieces, least, top_value):
    loudness = 1.0
    for position, blocks in pieces:
        draws = jax.random.uniform(jax.random.fold_in(jax.random.fold_in(own_key, 6), position), (blocks,), jnp.float32, least / len(pieces), top_value / len(pieces))
        loudness = loudness * jnp.repeat(jnp.exp(draws), dims[position] // blocks).reshape((-1,) + (1,) * (len(dims) - 1 - position))
    return loudness


def gaussian(stream_key, shape, width, most, shards=(), kind=jnp.bfloat16):
    entries = jax.random.normal(stream_key, shape, jnp.float32) * width
    if len(shards) > 0:
        entries = block_levels(stream_key, shape, shards, -0.22, 0.18) * entries
    return jnp.clip(entries, min=-most, max=most).astype(kind)


def setup_inputs(seed: int = 0) -> dict:
    seeds = jax.random.split(jax.random.key(seed), 7)
    return {
        "pixel_row": draw_pixel_row(jax.random.fold_in(seeds[6], 71), 0),
        "pixel_col": draw_pixel_col(jax.random.fold_in(seeds[6], 71), 0),
        "strip_of_span": draw_strip_of_span(jax.random.fold_in(seeds[6], 71), 0),
        "shear_one": gaussian(seeds[3], (SPANS, GAL), 1.0, 6.0, ((0, 128),), jnp.float32),
        "shear_two": gaussian(seeds[4], (SPANS, GAL), 1.0, 6.0, ((0, 128),), jnp.float32),
        "weight": jnp.clip(jnp.exp(math.log(4.0) - 2.7725887 * jax.random.uniform(seeds[5], (SPANS, GAL), jnp.float32) ** block_levels(seeds[5], (SPANS, GAL), ((0, 128),), -0.2, 0.2)), 0.25, 4.0),
    }


def reference(pixel_row, pixel_col, strip_of_span, shear_one, shear_two, weight):
    span_count = pixel_row.shape[0]
    map_rows = SLAB * N_BLK
    map_cols = TILE_COLS * N_COL
    shard_size = strip_of_span.shape[1]
    shard_index = jnp.arange(span_count, dtype=jnp.int32) // shard_size
    strip_index = strip_of_span.reshape(-1).astype(jnp.int32)
    grid_row = strip_index[:, None] * STRIP + pixel_row
    grid_col = (shard_index % N_COL)[:, None] * TILE_COLS + pixel_col
    cell = (grid_row * map_cols + grid_col).astype(jnp.int32).reshape(-1)
    rounded_weight = lax.optimization_barrier(weight.astype(jnp.bfloat16)).astype(jnp.float32).reshape(-1)
    weighted_one = lax.optimization_barrier((weight * shear_one).astype(jnp.bfloat16)).astype(jnp.float32).reshape(-1)
    weighted_two = lax.optimization_barrier((weight * shear_two).astype(jnp.bfloat16)).astype(jnp.float32).reshape(-1)
    zeros_cells = jnp.zeros((map_rows * map_cols,), jnp.float32)
    weight_sum = zeros_cells.at[cell].add(rounded_weight)
    sum_one = zeros_cells.at[cell].add(weighted_one)
    sum_two = zeros_cells.at[cell].add(weighted_two)
    floored = jnp.maximum(weight_sum, 1.0)
    gamma_one = (sum_one / floored).reshape(map_rows, map_cols)
    gamma_two = (sum_two / floored).reshape(map_rows, map_cols)
    spectrum = jnp.fft.fft2(lax.complex(gamma_one, gamma_two))
    freq_x = jnp.fft.fftfreq(map_cols).astype(jnp.float32)[None, :]
    freq_y = jnp.fft.fftfreq(map_rows).astype(jnp.float32)[:, None]
    radius_sq = freq_x * freq_x + freq_y * freq_y
    safe_radius = jnp.where(radius_sq > 0, radius_sq, 1.0)
    kernel_re = (freq_x * freq_x - freq_y * freq_y) / safe_radius
    kernel_im = 2.0 * freq_x * freq_y / safe_radius
    spec_re = jnp.real(spectrum)
    spec_im = jnp.imag(spectrum)
    hat_re = kernel_re * spec_re + kernel_im * spec_im
    hat_im = kernel_re * spec_im - kernel_im * spec_re
    convergence = jnp.fft.ifft2(lax.complex(hat_re, hat_im))
    return jnp.real(convergence).astype(jnp.float32), jnp.imag(convergence).astype(jnp.float32)
```

```python
import math

import jax
import jax.numpy as jnp
import numpy as np
from jax import lax
from jax.experimental import pallas as pl
from jax.experimental.pallas import tpu as pltpu
from jax.sharding import PartitionSpec as P

N = 8192
DEV = 128
F32 = jnp.float32
BF16 = jnp.bfloat16
VMEM = pl.BlockSpec(memory_space=pltpu.VMEM)
SMEM = pl.BlockSpec(memory_space=pltpu.SMEM)


def split_table(table):
    high = table.astype(BF16)
    low = (table - high.astype(np.float64)).astype(BF16)
    return jnp.asarray(high), jnp.asarray(low)


def real_form(angle):
    c, s = np.cos(angle), np.sin(angle)
    return np.stack([np.stack([c, s], 1), np.stack([-s, c], 1)], 0)


def row_table():
    b = np.arange(128)[:, None]
    q = np.arange(128)[None, :]
    m = real_form(-2 * np.pi * (b * q % 128) / 128)
    m = m.reshape(2, 128, 2, 2, 2, 32)
    return m.transpose(0, 1, 4, 3, 2, 5).reshape(256, 256)


def row_inverse_table():
    q = np.arange(128)[:, None]
    b = np.arange(128)[None, :]
    m = real_form(2 * np.pi * (b * q % 128) / 128)
    m = m.reshape(2, 2, 2, 32, 2, 128)
    return m.transpose(2, 1, 0, 3, 4, 5).reshape(256, 256)


def col_table(sign):
    b = np.arange(64)[:, None]
    q = np.arange(64)[None, :]
    m = real_form(sign * 2 * np.pi * (b * q % 64) / 64)
    full = np.zeros((2, 2, 64, 2, 2, 64))
    for par in range(2):
        full[:, par, :, :, par, :] = m
    return full.reshape(256, 256)


def twiddle_table(rows, lanes, sign, factor):
    r = np.arange(rows)[:, None]
    angle = sign * 2 * np.pi * (r * lanes[None, :] % N) / N
    return (
        jnp.asarray(factor * np.cos(angle), F32),
        jnp.asarray(factor * np.sin(angle), F32),
    )


def times(value, k, n, sign):
    re, im = value
    k = k % n
    if k == 0:
        return re, im
    if 4 * k == n:
        return (im, -re) if sign < 0 else (-im, re)
    if 2 * k == n:
        return -re, -im
    if 4 * k == 3 * n:
        return (-im, re) if sign < 0 else (im, -re)
    c = math.cos(2 * math.pi * k / n)
    s = sign * math.sin(2 * math.pi * k / n)
    if 8 * k == n or 8 * k == 5 * n or 8 * k == 3 * n or 8 * k == 7 * n:
        root = math.sqrt(0.5)
        sc = 1.0 if c > 0 else -1.0
        ss = 1.0 if s > 0 else -1.0
        if sc == ss:
            return (re - im) * (sc * root), (re + im) * (sc * root)
        return (re + im) * (sc * root), (im - re) * (sc * root)
    return re * c - im * s, re * s + im * c


def small_dft(values, sign):
    n = len(values)
    if n == 1:
        return values
    even = small_dft(values[0::2], sign)
    odd = small_dft(values[1::2], sign)
    low, high = [], []
    for k in range(n // 2):
        er, ei = even[k]
        tr, ti = times(odd[k], k, n, sign)
        low.append((er + tr, ei + ti))
        high.append((er - tr, ei - ti))
    return low + high


def major_dft(load, store, scratch, first, second, sign):
    n = first * second
    for i0 in range(second):
        out = small_dft([load(second * i1 + i0) for i1 in range(first)], sign)
        for o0 in range(first):
            re, im = times(out[o0], i0 * o0, n, sign)
            scratch[0, o0 * second + i0] = re
            scratch[1, o0 * second + i0] = im
    for o0 in range(first):
        vals = [(scratch[0, o0 * second + i0], scratch[1, o0 * second + i0]) for i0 in range(second)]
        out = small_dft(vals, sign)
        for o1 in range(second):
            store(o0 + first * o1, out[o1])


def dot(a, b):
    return jnp.dot(a, b, preferred_element_type=F32)


def dot3(x, high, low):
    xh = x.astype(BF16)
    xl = (x - xh.astype(F32)).astype(BF16)
    return dot(xh, high) + dot(xl, high) + dot(xh, low)


def pack_kernel(row_ref, col_ref, strip_ref, one_ref, two_ref, w_ref, out_ref):
    strip = strip_ref[...].astype(F32)
    along = jnp.broadcast_to(strip, (256, 256))
    down = along.T
    i = lax.broadcasted_iota(jnp.int32, (256, 256), 0)
    j = lax.broadcasted_iota(jnp.int32, (256, 256), 1)
    earlier = jnp.where((along == down) & (i < j), 1.0, 0.0)
    place = 2.0 * strip + jnp.sum(earlier, axis=0, keepdims=True)
    pick = (place.astype(jnp.int32) == i).astype(BF16)
    w = w_ref[...]
    row = row_ref[...]
    col = col_ref[...]
    block = col // 128
    a = (row * 4 + block % 4 + 1) * jnp.where(block >= 8, -1, 1)
    b = col % 128 + 128 * (block // 4 % 2)
    fields = [
        w.astype(BF16),
        (w * one_ref[...]).astype(BF16),
        (w * two_ref[...]).astype(BF16),
        a.astype(F32).astype(BF16),
        b.astype(F32).astype(BF16),
    ]
    for f in range(5):
        out_ref[:, f * 256 : (f + 1) * 256] = dot(pick, fields[f]).astype(BF16)


def row_kernel(
    band_ref, block_ref, in_ref, tc_ref, ts_ref, wh_ref, wl_ref, out_ref, acc_ref, scr_ref, mid_ref
):
    acc_ref[...] = jnp.zeros_like(acc_ref)
    lane_iota = lax.broadcasted_iota(jnp.int32, (128, 256), 0)
    row_iota = lax.broadcasted_iota(jnp.int32, (8, 256), 0)

    def bin_group(g, carry):
        start = pl.multiple_of(g * 16, 16)
        data = in_ref[pl.ds(start, 16), :].astype(F32)
        a = (jnp.abs(data[:, 768:1024]) - 1.0).astype(jnp.int32)
        row8 = (a >> 2) & 7
        col128 = data[:, 1024:1280].astype(jnp.int32) & 127
        for k in range(16):
            hot = row8[k : k + 1] == row_iota
            lhs = jnp.concatenate(
                [jnp.where(hot, data[k : k + 1, f * 256 : (f + 1) * 256], 0.0) for f in range(3)], 0
            ).astype(BF16)
            cols = jnp.where(col128[k : k + 1] == lane_iota, 1.0, 0.0).astype(BF16)
            part = lax.dot_general(lhs, cols, (((1,), (1,)), ((), ())), preferred_element_type=F32)
            band = pl.multiple_of(band_ref[start + k] * 8, 8)
            block = block_ref[start + k]
            for f in range(3):
                acc_ref[f, block, pl.ds(band, 8), :] += part[f * 8 : f * 8 + 8]
        return carry

    lax.fori_loop(0, 16, bin_group, 0)

    def row_group(g, carry):
        rows = pl.ds(pl.multiple_of(g * 8, 8), 8)

        def load(i):
            scale = 1.0 / jnp.maximum(acc_ref[0, i, rows, :], 1.0)
            return acc_ref[1, i, rows, :] * scale, acc_ref[2, i, rows, :] * scale

        def store(p, value):
            re, im = value
            c, s = tc_ref[p : p + 1, :], ts_ref[p : p + 1, :]
            mid_ref[p, rows, 0:128] = re * c - im * s
            mid_ref[p, rows, 128:256] = re * s + im * c

        major_dft(load, store, scr_ref, 8, 8, -1)
        return carry

    lax.fori_loop(0, 8, row_group, 0)

    def mix(g, carry):
        p = g * 4
        lhs = mid_ref[pl.ds(p, 4), :, :].reshape(256, 256)
        out = dot3(lhs, wh_ref[...], wl_ref[...])
        for k in range(4):
            part = out[64 * k : 64 * k + 64]
            turned = jnp.concatenate([part[:, 0:128], part[:, 128:256]], 0).T
            out_ref[pl.ds(2 * (p + k), 2), :, :] = turned.astype(BF16).reshape(2, 64, 128)
        return carry

    lax.fori_loop(0, 16, mix, 0)


def col_kernel(
    me_ref, in_ref, tc_ref, ts_ref, fh_ref, fl_ref, gh_ref, gl_ref, out_ref, scr_ref, mid_ref
):
    me = me_ref[0]

    def forward(g, carry):
        rows = pl.ds(pl.multiple_of(g * 8, 8), 8)
        rows_im = pl.ds(pl.multiple_of(g * 8 + 32, 8), 8)

        def load(i):
            return in_ref[i, rows, :].astype(F32), in_ref[i, rows_im, :].astype(F32)

        def store(p, value):
            re, im = value
            c, s = tc_ref[p : p + 1, :], ts_ref[p : p + 1, :]
            mid_ref[p, rows, 0:128] = re * c - im * s
            mid_ref[p, rows, 128:256] = re * s + im * c

        major_dft(load, store, scr_ref, 8, 16, -1)
        return carry

    lax.fori_loop(0, 4, forward, 0)

    sub = lax.broadcasted_iota(jnp.int32, (32, 128), 0)
    lane = lax.broadcasted_iota(jnp.int32, (32, 128), 1)
    v = me // 2 + 64 * (64 * (me % 2) + 32 * (lane // 64) + sub)
    fx = jnp.where(v < N // 2, v, v - N).astype(F32) * (1.0 / N)
    fx2 = fx * fx

    def mix(g, carry):
        p0 = g * 8
        lhs = mid_ref[pl.ds(p0, 8), :, :].reshape(256, 256)
        spec = dot3(lhs, fh_ref[...], fl_ref[...])
        parts = []
        for k in range(8):
            re, im = spec[32 * k : 32 * k + 32, 0:128], spec[32 * k : 32 * k + 32, 128:256]
            u = p0 + k + 128 * (lane % 64)
            fy = jnp.where(u < N // 2, u, u - N).astype(F32) * (1.0 / N)
            fy2 = fy * fy
            q = fx2 + fy2
            inv = 1.0 / jnp.where(q > 0, q, 1.0)
            kr = (fx2 - fy2) * inv
            ki = 2.0 * fx * fy * inv
            parts.append(jnp.concatenate([kr * re + ki * im, kr * im - ki * re], 1))
        hat = jnp.concatenate(parts, 0)
        back = dot3(hat, gh_ref[...], gl_ref[...])
        for k in range(8):
            re, im = back[32 * k : 32 * k + 32, 0:128], back[32 * k : 32 * k + 32, 128:256]
            c, s = tc_ref[pl.ds(p0 + k, 1), :], ts_ref[pl.ds(p0 + k, 1), :]
            mid_ref[p0 + k, :, 0:128] = (re * c + im * s) * (1.0 / N)
            mid_ref[p0 + k, :, 128:256] = (im * c - re * s) * (1.0 / N)
        return carry

    lax.fori_loop(0, 16, mix, 0)

    def inverse(g, carry):
        rows = pl.ds(pl.multiple_of(g * 8, 8), 8)
        rows_im = pl.ds(pl.multiple_of(g * 8 + 32, 8), 8)

        def load(i):
            return mid_ref[i, rows, 0:128], mid_ref[i, rows, 128:256]

        def store(a, value):
            re, im = value
            out_ref[a, rows, :] = re.astype(BF16)
            out_ref[a, rows_im, :] = im.astype(BF16)

        major_dft(load, store, scr_ref, 8, 16, 1)
        return carry

    lax.fori_loop(0, 4, inverse, 0)


def back_kernel(in_ref, tc_ref, ts_ref, wh_ref, wl_ref, e_ref, b_ref, scr_ref, mid_ref):
    def mix(g, carry):
        p = g * 4
        pieces = []
        for k in range(4):
            part = in_ref[pl.ds(2 * (p + k), 2), :, :].reshape(128, 128).astype(F32).T
            pieces.append(jnp.concatenate([part[0:64], part[64:128]], 1))
        lhs = jnp.concatenate(pieces, 0).astype(BF16)
        out = dot(lhs, wh_ref[...]) + dot(lhs, wl_ref[...])
        for k in range(4):
            re, im = out[64 * k : 64 * k + 64, 0:128], out[64 * k : 64 * k + 64, 128:256]
            c, s = tc_ref[pl.ds(p + k, 1), :], ts_ref[pl.ds(p + k, 1), :]
            mid_ref[p + k, :, 0:128] = re * c - im * s
            mid_ref[p + k, :, 128:256] = re * s + im * c
        return carry

    lax.fori_loop(0, 16, mix, 0)

    def row_group(g, carry):
        rows = pl.ds(pl.multiple_of(g * 8, 8), 8)

        def load(i):
            return mid_ref[i, rows, 0:128], mid_ref[i, rows, 128:256]

        def store(a, value):
            e_ref[rows, a * 128 : a * 128 + 128] = value[0]
            b_ref[rows, a * 128 : a * 128 + 128] = value[1]

        major_dft(load, store, scr_ref, 8, 8, 1)
        return carry

    lax.fori_loop(0, 8, row_group, 0)


def exchange(x):
    return lax.all_to_all(x, ("blk", "col"), split_axis=0, concat_axis=0, tiled=True)


def pack_call(pixel_row, pixel_col, strip_of_span, shear_one, shear_two, weight):
    return pl.pallas_call(
        pack_kernel,
        out_shape=jax.ShapeDtypeStruct((256, 1280), BF16),
        in_specs=[VMEM] * 6,
        out_specs=VMEM,
        name="pack",
    )(pixel_row, pixel_col, strip_of_span, shear_one, shear_two, weight)


def row_call(got):
    tags = got[:, 768].astype(F32)
    high = got[:, 1024].astype(F32)
    a = (jnp.abs(tags) - 1.0).astype(jnp.int32)
    band = a // 32
    tile = jnp.arange(256, dtype=jnp.int32) // 2 % 4
    block = tile * 16 + a % 4 + jnp.where(high >= 128.0, 4, 0) + jnp.where(tags < 0, 8, 0)
    tc, ts = twiddle_table(64, np.arange(128), -1, 1.0)
    wh, wl = split_table(row_table())
    return pl.pallas_call(
        row_kernel,
        out_shape=jax.ShapeDtypeStruct((DEV, 64, 128), BF16),
        in_specs=[SMEM, SMEM] + [VMEM] * 5,
        out_specs=VMEM,
        scratch_shapes=[
            pltpu.VMEM((3, 64, 64, 128), F32),
            pltpu.VMEM((2, 64, 8, 128), F32),
            pltpu.VMEM((64, 64, 256), F32),
        ],
        name="rows",
    )(band, block, got, tc, ts, wh, wl)


def col_call(me, x):
    tc, ts = twiddle_table(128, np.arange(128) % 64, -1, 1.0)
    fh, fl = split_table(col_table(-1))
    gh, gl = split_table(col_table(1))
    return pl.pallas_call(
        col_kernel,
        out_shape=jax.ShapeDtypeStruct((DEV, 64, 128), BF16),
        in_specs=[SMEM] + [VMEM] * 7,
        out_specs=VMEM,
        scratch_shapes=[pltpu.VMEM((2, 128, 8, 128), F32), pltpu.VMEM((128, 32, 256), F32)],
        name="columns",
    )(me, x, tc, ts, fh, fl, gh, gl)


def back_call(x):
    tc, ts = twiddle_table(64, np.arange(128), 1, 1.0 / N)
    wh, wl = split_table(row_inverse_table())
    return pl.pallas_call(
        back_kernel,
        out_shape=(jax.ShapeDtypeStruct((64, N), F32), jax.ShapeDtypeStruct((64, N), F32)),
        in_specs=[VMEM] * 5,
        out_specs=(VMEM, VMEM),
        scratch_shapes=[pltpu.VMEM((2, 64, 8, 128), F32), pltpu.VMEM((64, 64, 256), F32)],
        name="back",
    )(x, tc, ts, wh, wl)


def local(pixel_row, pixel_col, strip_of_span, shear_one, shear_two, weight):
    me = (lax.axis_index("blk") * lax.axis_size("col") + lax.axis_index("col")).reshape(1)
    sent = pack_call(pixel_row, pixel_col, strip_of_span, shear_one, shear_two, weight)
    got = exchange(sent.reshape(DEV, 2, 1280)).reshape(256, 1280)
    columns = exchange(row_call(got))
    rows = exchange(col_call(me.astype(jnp.int32), columns))
    return back_call(rows)


def solution(mesh):
    placed = (P(("blk", "col"), None),) * 6
    return jax.shard_map(
        local,
        mesh=mesh,
        in_specs=placed,
        out_specs=(P(("blk", "col"), None), P(("blk", "col"), None)),
        check_vma=False,
    )
```

```python
import math

import jax
import jax.numpy as jnp
import numpy as np
from jax import lax
from jax.experimental import pallas as pl
from jax.experimental.pallas import tpu as pltpu
from jax.sharding import PartitionSpec as P

N = 8192
DEV = 128
LIMIT = 40 << 20
F32 = jnp.float32
BF16 = jnp.bfloat16
F8 = jnp.float8_e4m3fn
VMEM = pl.BlockSpec(memory_space=pltpu.VMEM)
SMEM = pl.BlockSpec(memory_space=pltpu.SMEM)
HBM = pl.BlockSpec(memory_space=pl.ANY)


def split_table(table):
    high = table.astype(BF16)
    low = (table - high.astype(np.float64)).astype(BF16)
    return jnp.asarray(high), jnp.asarray(low)


def real_form(angle):
    c, s = np.cos(angle), np.sin(angle)
    return np.stack([np.stack([c, s], 1), np.stack([-s, c], 1)], 0)


def row_table():
    b = np.arange(128)[:, None]
    q = np.arange(128)[None, :]
    m = real_form(-2 * np.pi * (b * q % 128) / 128)
    m = m.reshape(2, 128, 2, 2, 2, 32)
    return m.transpose(0, 1, 4, 3, 2, 5).reshape(256, 256)


def row_inverse_table():
    q = np.arange(128)[:, None]
    b = np.arange(128)[None, :]
    m = real_form(2 * np.pi * (b * q % 128) / 128)
    m = m.reshape(2, 2, 2, 32, 2, 128)
    return m.transpose(2, 1, 0, 3, 4, 5).reshape(256, 256)


def col_table(sign):
    b = np.arange(64)[:, None]
    q = np.arange(64)[None, :]
    m = real_form(sign * 2 * np.pi * (b * q % 64) / 64)
    full = np.zeros((2, 2, 64, 2, 2, 64))
    for par in range(2):
        full[:, par, :, :, par, :] = m
    return full.reshape(256, 256)


def twiddle_table(rows, lanes, sign, factor):
    r = np.arange(rows)[:, None]
    angle = sign * 2 * np.pi * (r * lanes[None, :] % N) / N
    return (
        jnp.asarray(factor * np.cos(angle), F32),
        jnp.asarray(factor * np.sin(angle), F32),
    )


def times(value, k, n, sign):
    re, im = value
    k = k % n
    if k == 0:
        return re, im
    if 4 * k == n:
        return (im, -re) if sign < 0 else (-im, re)
    if 2 * k == n:
        return -re, -im
    if 4 * k == 3 * n:
        return (-im, re) if sign < 0 else (im, -re)
    c = math.cos(2 * math.pi * k / n)
    s = sign * math.sin(2 * math.pi * k / n)
    if 8 * k == n or 8 * k == 5 * n or 8 * k == 3 * n or 8 * k == 7 * n:
        root = math.sqrt(0.5)
        sc = 1.0 if c > 0 else -1.0
        ss = 1.0 if s > 0 else -1.0
        if sc == ss:
            return (re - im) * (sc * root), (re + im) * (sc * root)
        return (re + im) * (sc * root), (im - re) * (sc * root)
    return re * c - im * s, re * s + im * c


def small_dft(values, sign):
    n = len(values)
    if n == 1:
        return values
    even = small_dft(values[0::2], sign)
    odd = small_dft(values[1::2], sign)
    low, high = [], []
    for k in range(n // 2):
        er, ei = even[k]
        tr, ti = times(odd[k], k, n, sign)
        low.append((er + tr, ei + ti))
        high.append((er - tr, ei - ti))
    return low + high


def major_dft(load, store, scratch, first, second, sign):
    n = first * second
    for i0 in range(second):
        out = small_dft([load(second * i1 + i0) for i1 in range(first)], sign)
        for o0 in range(first):
            re, im = times(out[o0], i0 * o0, n, sign)
            scratch[0, o0 * second + i0] = re
            scratch[1, o0 * second + i0] = im
    for o0 in range(first):
        vals = [(scratch[0, o0 * second + i0], scratch[1, o0 * second + i0]) for i0 in range(second)]
        out = small_dft(vals, sign)
        for o1 in range(second):
            store(o0 + first * o1, out[o1])


def dot(a, b):
    return jnp.dot(a, b, preferred_element_type=F32)


def dot3(x, high, low):
    xh = x.astype(BF16)
    xl = (x - xh.astype(F32)).astype(BF16)
    return dot(xh, high) + dot(xl, high) + dot(xh, low)


def pack_kernel(row_ref, col_ref, strip_ref, one_ref, two_ref, w_ref, out_ref):
    strip = strip_ref[...].astype(F32)
    along = jnp.broadcast_to(strip, (256, 256))
    down = along.T
    i = lax.broadcasted_iota(jnp.int32, (256, 256), 0)
    j = lax.broadcasted_iota(jnp.int32, (256, 256), 1)
    earlier = jnp.where((along == down) & (i < j), 1.0, 0.0)
    place = 2.0 * strip + jnp.sum(earlier, axis=0, keepdims=True)
    pick = (place.astype(jnp.int32) == i).astype(BF16)
    w = w_ref[...]
    row = row_ref[...]
    col = col_ref[...]
    block = col // 128
    a = (row * 4 + block % 4 + 1) * jnp.where(block >= 8, -1, 1)
    b = col % 128 + 128 * (block // 4 % 2)
    fields = [
        w.astype(BF16),
        (w * one_ref[...]).astype(BF16),
        (w * two_ref[...]).astype(BF16),
        a.astype(F32).astype(BF16),
        b.astype(F32).astype(BF16),
    ]
    for f in range(5):
        out_ref[:, :, f * 256 : (f + 1) * 256] = dot(pick, fields[f]).astype(BF16).reshape(128, 2, 256)


def row_kernel(
    band_ref, block_ref, in_ref, tc_ref, ts_ref, wh_ref, wl_ref, out_ref, acc_ref, scr_ref, mid_ref
):
    acc_ref[...] = jnp.zeros_like(acc_ref)
    lane_iota = lax.broadcasted_iota(jnp.int32, (128, 256), 0)
    row_iota = lax.broadcasted_iota(jnp.int32, (8, 256), 0)

    def bin_group(g, carry):
        start = pl.multiple_of(g * 16, 16)
        data = in_ref[pl.ds(start, 16), :].astype(F32)
        a = (jnp.abs(data[:, 768:1024]) - 1.0).astype(jnp.int32)
        row8 = (a >> 2) & 7
        col128 = data[:, 1024:1280].astype(jnp.int32) & 127
        for k in range(16):
            hot = row8[k : k + 1] == row_iota
            lhs = jnp.concatenate(
                [jnp.where(hot, data[k : k + 1, f * 256 : (f + 1) * 256], 0.0) for f in range(3)], 0
            ).astype(BF16)
            cols = jnp.where(col128[k : k + 1] == lane_iota, 1.0, 0.0).astype(F8)
            part = lax.dot_general(lhs, cols, (((1,), (1,)), ((), ())), preferred_element_type=F32)
            band = pl.multiple_of(band_ref[start + k] * 8, 8)
            block = block_ref[start + k]
            for f in range(3):
                acc_ref[f, block, pl.ds(band, 8), :] += part[f * 8 : f * 8 + 8]
        return carry

    lax.fori_loop(0, 16, bin_group, 0)

    def row_group(g, carry):
        rows = pl.ds(pl.multiple_of(g * 8, 8), 8)

        def load(i):
            scale = 1.0 / jnp.maximum(acc_ref[0, i, rows, :], 1.0)
            return acc_ref[1, i, rows, :] * scale, acc_ref[2, i, rows, :] * scale

        def store(p, value):
            re, im = value
            c, s = tc_ref[p : p + 1, :], ts_ref[p : p + 1, :]
            mid_ref[p, rows, 0:128] = re * c - im * s
            mid_ref[p, rows, 128:256] = re * s + im * c

        major_dft(load, store, scr_ref, 8, 8, -1)
        return carry

    lax.fori_loop(0, 8, row_group, 0)

    def mix(g, carry):
        p = g * 4
        lhs = mid_ref[pl.ds(p, 4), :, :].reshape(256, 256)
        out = dot3(lhs, wh_ref[...], wl_ref[...])
        for k in range(4):
            part = out[64 * k : 64 * k + 64]
            turned = jnp.concatenate([part[:, 0:128], part[:, 128:256]], 0).T
            out_ref[pl.ds(2 * (p + k), 2), :, :] = turned.astype(BF16).reshape(2, 64, 128)
        return carry

    lax.fori_loop(0, 16, mix, 0, unroll=8)


def col_kernel(
    me_ref, in_ref, tc_ref, ts_ref, fh_ref, fl_ref, gh_ref, gl_ref, out_ref, scr_ref, mid_ref
):
    me = me_ref[0]

    def forward(g, carry):
        rows = pl.ds(pl.multiple_of(g * 8, 8), 8)
        rows_im = pl.ds(pl.multiple_of(g * 8 + 32, 8), 8)

        def load(i):
            return in_ref[i, rows, :].astype(F32), in_ref[i, rows_im, :].astype(F32)

        def store(p, value):
            re, im = value
            c, s = tc_ref[p : p + 1, :], ts_ref[p : p + 1, :]
            mid_ref[p, rows, 0:128] = re * c - im * s
            mid_ref[p, rows, 128:256] = re * s + im * c

        major_dft(load, store, scr_ref, 8, 16, -1)
        return carry

    lax.fori_loop(0, 4, forward, 0)

    sub = lax.broadcasted_iota(jnp.int32, (32, 128), 0)
    lane = lax.broadcasted_iota(jnp.int32, (32, 128), 1)
    v = me // 2 + 64 * (64 * (me % 2) + 32 * (lane // 64) + sub)
    fx = jnp.where(v < N // 2, v, v - N).astype(F32) * (1.0 / N)
    fx2 = fx * fx

    def mix(g, carry):
        p0 = g * 8
        lhs = mid_ref[pl.ds(p0, 8), :, :].reshape(256, 256)
        spec = dot3(lhs, fh_ref[...], fl_ref[...])
        parts = []
        for k in range(8):
            re, im = spec[32 * k : 32 * k + 32, 0:128], spec[32 * k : 32 * k + 32, 128:256]
            u = p0 + k + 128 * (lane % 64)
            fy = jnp.where(u < N // 2, u, u - N).astype(F32) * (1.0 / N)
            fy2 = fy * fy
            q = fx2 + fy2
            inv = 1.0 / jnp.where(q > 0, q, 1.0)
            kr = (fx2 - fy2) * inv
            ki = 2.0 * fx * fy * inv
            parts.append(jnp.concatenate([kr * re + ki * im, kr * im - ki * re], 1))
        hat = jnp.concatenate(parts, 0)
        back = dot3(hat, gh_ref[...], gl_ref[...])
        for k in range(8):
            re, im = back[32 * k : 32 * k + 32, 0:128], back[32 * k : 32 * k + 32, 128:256]
            c, s = tc_ref[pl.ds(p0 + k, 1), :], ts_ref[pl.ds(p0 + k, 1), :]
            mid_ref[p0 + k, :, 0:128] = (re * c + im * s) * (1.0 / N)
            mid_ref[p0 + k, :, 128:256] = (im * c - re * s) * (1.0 / N)
        return carry

    lax.fori_loop(0, 16, mix, 0, unroll=8)

    def inverse(g, carry):
        rows = pl.ds(pl.multiple_of(g * 8, 8), 8)
        rows_im = pl.ds(pl.multiple_of(g * 8 + 32, 8), 8)

        def load(i):
            return mid_ref[i, rows, 0:128], mid_ref[i, rows, 128:256]

        def store(a, value):
            re, im = value
            out_ref[a, rows, :] = re.astype(BF16)
            out_ref[a, rows_im, :] = im.astype(BF16)

        major_dft(load, store, scr_ref, 8, 16, 1)
        return carry

    lax.fori_loop(0, 4, inverse, 0)


def back_kernel(
    in_ref, tc_ref, ts_ref, wh_ref, wl_ref, e_hbm, b_hbm, scr_ref, mid_ref, e_ref, b_ref, sems
):
    def leave(g, which):
        rows = pl.ds(pl.multiple_of(g * 8, 8), 8)
        source, target = ((e_ref, e_hbm), (b_ref, b_hbm))[which]
        return pltpu.make_async_copy(source.at[rows], target.at[rows], sems.at[g, which])

    def mix(g, carry):
        p = g * 4
        pieces = []
        for k in range(4):
            part = in_ref[pl.ds(2 * (p + k), 2), :, :].reshape(128, 128).astype(F32).T
            pieces.append(jnp.concatenate([part[0:64], part[64:128]], 1))
        lhs = jnp.concatenate(pieces, 0).astype(BF16)
        out = dot(lhs, wh_ref[...]) + dot(lhs, wl_ref[...])
        for k in range(4):
            re, im = out[64 * k : 64 * k + 64, 0:128], out[64 * k : 64 * k + 64, 128:256]
            c, s = tc_ref[pl.ds(p + k, 1), :], ts_ref[pl.ds(p + k, 1), :]
            mid_ref[p + k, :, 0:128] = re * c - im * s
            mid_ref[p + k, :, 128:256] = re * s + im * c
        return carry

    lax.fori_loop(0, 16, mix, 0, unroll=8)

    def row_group(g, carry):
        rows = pl.ds(pl.multiple_of(g * 8, 8), 8)

        def load(i):
            return mid_ref[i, rows, 0:128], mid_ref[i, rows, 128:256]

        def store(a, value):
            e_ref[rows, a * 128 : a * 128 + 128] = value[0]
            b_ref[rows, a * 128 : a * 128 + 128] = value[1]

        major_dft(load, store, scr_ref, 8, 8, 1)
        leave(g, 0).start()
        leave(g, 1).start()
        return carry

    lax.fori_loop(0, 8, row_group, 0)
    for g in range(8):
        leave(g, 0).wait()
        leave(g, 1).wait()


def exchange(x):
    return lax.all_to_all(x, ("blk", "col"), split_axis=0, concat_axis=0, tiled=True)


def on_chip(x):
    return pltpu.with_memory_space_constraint(x, pltpu.VMEM)


def pack_call(pixel_row, pixel_col, strip_of_span, shear_one, shear_two, weight):
    return pl.pallas_call(
        pack_kernel,
        out_shape=pltpu.VMEM((128, 2, 1280), BF16),
        in_specs=[VMEM] * 6,
        out_specs=VMEM,
        compiler_params=pltpu.CompilerParams(vmem_limit_bytes=LIMIT),
        name="pack",
    )(pixel_row, pixel_col, strip_of_span, shear_one, shear_two, weight)


def row_call(got):
    tags = got[:, 768].astype(F32)
    high = got[:, 1024].astype(F32)
    a = (jnp.abs(tags) - 1.0).astype(jnp.int32)
    band = a // 32
    tile = jnp.arange(256, dtype=jnp.int32) // 2 % 4
    block = tile * 16 + a % 4 + jnp.where(high >= 128.0, 4, 0) + jnp.where(tags < 0, 8, 0)
    tc, ts = twiddle_table(64, np.arange(128), -1, 1.0)
    wh, wl = split_table(row_table())
    return pl.pallas_call(
        row_kernel,
        out_shape=pltpu.VMEM((DEV, 64, 128), BF16),
        in_specs=[SMEM, SMEM] + [VMEM] * 5,
        out_specs=VMEM,
        scratch_shapes=[
            pltpu.VMEM((3, 64, 64, 128), F32),
            pltpu.VMEM((2, 64, 8, 128), F32),
            pltpu.VMEM((64, 64, 256), F32),
        ],
        compiler_params=pltpu.CompilerParams(vmem_limit_bytes=LIMIT),
        name="rows",
    )(band, block, got, tc, ts, wh, wl)


def col_call(me, x):
    tc, ts = twiddle_table(128, np.arange(128) % 64, -1, 1.0)
    fh, fl = split_table(col_table(-1))
    gh, gl = split_table(col_table(1))
    return pl.pallas_call(
        col_kernel,
        out_shape=pltpu.VMEM((DEV, 64, 128), BF16),
        in_specs=[SMEM] + [VMEM] * 7,
        out_specs=VMEM,
        scratch_shapes=[pltpu.VMEM((2, 128, 8, 128), F32), pltpu.VMEM((128, 32, 256), F32)],
        compiler_params=pltpu.CompilerParams(vmem_limit_bytes=LIMIT),
        name="columns",
    )(me, x, tc, ts, fh, fl, gh, gl)


def back_call(x):
    tc, ts = twiddle_table(64, np.arange(128), 1, 1.0 / N)
    wh, wl = split_table(row_inverse_table())
    return pl.pallas_call(
        back_kernel,
        out_shape=(jax.ShapeDtypeStruct((64, N), F32), jax.ShapeDtypeStruct((64, N), F32)),
        in_specs=[VMEM] * 5,
        out_specs=(HBM, HBM),
        scratch_shapes=[
            pltpu.VMEM((2, 64, 8, 128), F32),
            pltpu.VMEM((64, 64, 256), F32),
            pltpu.VMEM((64, N), F32),
            pltpu.VMEM((64, N), F32),
            pltpu.SemaphoreType.DMA((8, 2)),
        ],
        compiler_params=pltpu.CompilerParams(vmem_limit_bytes=LIMIT),
        name="back",
    )(x, tc, ts, wh, wl)


def local(pixel_row, pixel_col, strip_of_span, shear_one, shear_two, weight):
    me = (lax.axis_index("blk") * lax.axis_size("col") + lax.axis_index("col")).reshape(1)
    me, pixel_row = lax.optimization_barrier((me.astype(jnp.int32), pixel_row))
    sent = pack_call(pixel_row, pixel_col, strip_of_span, shear_one, shear_two, weight)
    got = exchange(sent).reshape(256, 1280)
    columns = exchange(row_call(got))
    rows = exchange(col_call(me, on_chip(columns)))
    return back_call(on_chip(rows))


def solution(mesh):
    placed = (P(("blk", "col"), None),) * 6
    return jax.shard_map(
        local,
        mesh=mesh,
        in_specs=placed,
        out_specs=(P(("blk", "col"), None), P(("blk", "col"), None)),
        check_vma=False,
    )
```

```python
import math

import jax
import jax.numpy as jnp
import numpy as np
from jax import lax
from jax.experimental import pallas as pl
from jax.experimental.pallas import tpu as pltpu
from jax.sharding import PartitionSpec as P

N = 8192
DEV = 128
LIMIT = 40 << 20
F32 = jnp.float32
BF16 = jnp.bfloat16
VMEM = pl.BlockSpec(memory_space=pltpu.VMEM)
SMEM = pl.BlockSpec(memory_space=pltpu.SMEM)
HBM = pl.BlockSpec(memory_space=pltpu.HBM)


def split_table(table):
    high = table.astype(BF16)
    low = (table - high.astype(np.float64)).astype(BF16)
    return jnp.asarray(high), jnp.asarray(low)


def real_form(angle):
    c, s = np.cos(angle), np.sin(angle)
    return np.stack([np.stack([c, s], 1), np.stack([-s, c], 1)], 0)


def row_table():
    b = np.arange(128)[:, None]
    q = np.arange(128)[None, :]
    m = real_form(-2 * np.pi * (b * q % 128) / 128)
    m = m.reshape(2, 128, 2, 2, 2, 32)
    return m.transpose(0, 1, 4, 3, 2, 5).reshape(256, 256)


def row_inverse_table():
    q = np.arange(128)[:, None]
    b = np.arange(128)[None, :]
    m = real_form(2 * np.pi * (b * q % 128) / 128)
    m = m.reshape(2, 2, 2, 32, 2, 128)
    return m.transpose(2, 1, 0, 3, 4, 5).reshape(256, 256)


def col_table(sign):
    b = np.arange(64)[:, None]
    q = np.arange(64)[None, :]
    m = real_form(sign * 2 * np.pi * (b * q % 64) / 64)
    full = np.zeros((2, 2, 64, 2, 2, 64))
    for par in range(2):
        full[:, par, :, :, par, :] = m
    return full.reshape(256, 256)


def twiddle_table(rows, lanes, sign, factor):
    r = np.arange(rows)[:, None]
    angle = sign * 2 * np.pi * (r * lanes[None, :] % N) / N
    return (
        jnp.asarray(factor * np.cos(angle), F32),
        jnp.asarray(factor * np.sin(angle), F32),
    )


def times(value, k, n, sign):
    re, im = value
    k = k % n
    if k == 0:
        return re, im
    if 4 * k == n:
        return (im, -re) if sign < 0 else (-im, re)
    if 2 * k == n:
        return -re, -im
    if 4 * k == 3 * n:
        return (-im, re) if sign < 0 else (im, -re)
    c = math.cos(2 * math.pi * k / n)
    s = sign * math.sin(2 * math.pi * k / n)
    if 8 * k == n or 8 * k == 5 * n or 8 * k == 3 * n or 8 * k == 7 * n:
        root = math.sqrt(0.5)
        sc = 1.0 if c > 0 else -1.0
        ss = 1.0 if s > 0 else -1.0
        if sc == ss:
            return (re - im) * (sc * root), (re + im) * (sc * root)
        return (re + im) * (sc * root), (im - re) * (sc * root)
    return re * c - im * s, re * s + im * c


def small_dft(values, sign):
    n = len(values)
    if n == 1:
        return values
    even = small_dft(values[0::2], sign)
    odd = small_dft(values[1::2], sign)
    low, high = [], []
    for k in range(n // 2):
        er, ei = even[k]
        tr, ti = times(odd[k], k, n, sign)
        low.append((er + tr, ei + ti))
        high.append((er - tr, ei - ti))
    return low + high


def major_dft(load, store, scratch, first, second, sign):
    n = first * second
    for i0 in range(second):
        out = small_dft([load(second * i1 + i0) for i1 in range(first)], sign)
        for o0 in range(first):
            re, im = times(out[o0], i0 * o0, n, sign)
            scratch[0, o0 * second + i0] = re
            scratch[1, o0 * second + i0] = im
    for o0 in range(first):
        vals = [(scratch[0, o0 * second + i0], scratch[1, o0 * second + i0]) for i0 in range(second)]
        out = small_dft(vals, sign)
        for o1 in range(second):
            store(o0 + first * o1, out[o1])


def dot(a, b):
    return jnp.dot(a, b, preferred_element_type=F32)


def dot3(x, high, low):
    xh = x.astype(BF16)
    xl = (x - xh.astype(F32)).astype(BF16)
    return dot(xh, high) + dot(xl, high) + dot(xh, low)


def pack_kernel(
    row_hbm, col_hbm, strip_hbm, one_hbm, two_hbm, w_hbm, out_ref, strip_ref, ints_ref, floats_ref, sems
):
    copies = [
        pltpu.make_async_copy(source, target, sems.at[i])
        for i, (source, target) in enumerate(
            [
                (strip_hbm, strip_ref),
                (w_hbm, floats_ref.at[0]),
                (one_hbm, floats_ref.at[1]),
                (two_hbm, floats_ref.at[2]),
                (row_hbm, ints_ref.at[0]),
                (col_hbm, ints_ref.at[1]),
            ]
        )
    ]
    for copy in copies:
        copy.start()
    copies[0].wait()
    strip = strip_ref[...].astype(F32)
    along = jnp.broadcast_to(strip, (256, 256))
    down = along.T
    i = lax.broadcasted_iota(jnp.int32, (256, 256), 0)
    j = lax.broadcasted_iota(jnp.int32, (256, 256), 1)
    earlier = jnp.where((along == down) & (i < j), 1.0, 0.0)
    place = 2.0 * strip + jnp.sum(earlier, axis=0, keepdims=True)
    pick = (place.astype(jnp.int32) == i).astype(BF16)

    def send(f, field):
        moved = dot(pick, field.astype(BF16)).astype(BF16)
        out_ref[:, :, f * 256 : (f + 1) * 256] = moved.reshape(128, 2, 256)

    copies[1].wait()
    w = floats_ref[0]
    send(0, w)
    copies[2].wait()
    send(1, w * floats_ref[1])
    copies[3].wait()
    send(2, w * floats_ref[2])
    copies[4].wait()
    copies[5].wait()
    row = ints_ref[0]
    col = ints_ref[1]
    block = col // 128
    a = (row * 4 + block % 4 + 1) * jnp.where(block >= 8, -1, 1)
    b = col % 128 + 128 * (block // 4 % 2)
    send(3, a.astype(F32))
    send(4, b.astype(F32))


def row_kernel(
    band_ref, block_ref, in_ref, tc_ref, ts_ref, wh_ref, wl_ref, out_ref, acc_ref, scr_ref, mid_ref
):
    acc_ref[...] = jnp.zeros_like(acc_ref)
    lane_iota = lax.broadcasted_iota(jnp.int32, (64, 256), 0).astype(F32).astype(BF16)
    row_iota = lax.broadcasted_iota(jnp.int32, (16, 256), 0).astype(F32).astype(BF16)
    one = jnp.ones((), BF16)
    none = jnp.zeros((), BF16)

    def bin_group(g, carry):
        start = pl.multiple_of(g * 16, 16)
        data = in_ref[pl.ds(start, 16), 0:768]
        tags = in_ref[pl.ds(start, 16), 768:1280].astype(F32)
        a = (jnp.abs(tags[:, 0:256]) - 1.0).astype(jnp.int32)
        b = tags[:, 256:512].astype(jnp.int32)
        high = (((a >> 2) & 7) + ((b >> 3) & 8)).astype(F32).astype(BF16)
        low = (b & 63).astype(F32).astype(BF16)
        for k in range(16):
            hot = jnp.broadcast_to(high[k : k + 1], (16, 256)) == row_iota
            lhs = jnp.concatenate(
                [
                    jnp.where(
                        hot,
                        jnp.broadcast_to(data[k : k + 1, f * 256 : (f + 1) * 256], (16, 256)),
                        none,
                    )
                    for f in range(3)
                ],
                0,
            )
            cols = jnp.where(jnp.broadcast_to(low[k : k + 1], (64, 256)) == lane_iota, one, none)
            part = lax.dot_general(lhs, cols, (((1,), (1,)), ((), ())), preferred_element_type=F32)
            band = pl.multiple_of(band_ref[start + k] * 8, 8)
            block = block_ref[start + k]
            for f in range(3):
                both = [part[f * 16 : f * 16 + 8], part[f * 16 + 8 : f * 16 + 16]]
                acc_ref[f, block, pl.ds(band, 8), :] += jnp.concatenate(both, 1)
        return carry

    lax.fori_loop(0, 16, bin_group, 0, unroll=8)

    def row_group(g, carry):
        rows = pl.ds(pl.multiple_of(g * 8, 8), 8)

        def load(i):
            scale = 1.0 / jnp.maximum(acc_ref[0, i, rows, :], 1.0)
            return acc_ref[1, i, rows, :] * scale, acc_ref[2, i, rows, :] * scale

        def store(p, value):
            re, im = value
            c, s = tc_ref[p : p + 1, :], ts_ref[p : p + 1, :]
            mid_ref[p, rows, 0:128] = re * c - im * s
            mid_ref[p, rows, 128:256] = re * s + im * c

        major_dft(load, store, scr_ref, 8, 8, -1)
        return carry

    lax.fori_loop(0, 8, row_group, 0)

    def mix(g, carry):
        p = g * 4
        lhs = mid_ref[pl.ds(p, 4), :, :].reshape(256, 256)
        out = dot3(lhs, wh_ref[...], wl_ref[...])
        for k in range(4):
            part = out[64 * k : 64 * k + 64]
            turned = jnp.concatenate([part[:, 0:128], part[:, 128:256]], 0).T
            out_ref[pl.ds(2 * (p + k), 2), :, :] = turned.astype(BF16).reshape(2, 64, 128)
        return carry

    lax.fori_loop(0, 16, mix, 0, unroll=16)


def col_kernel(
    me_ref, in_ref, tc_ref, ts_ref, fh_ref, fl_ref, gh_ref, gl_ref, out_ref, scr_ref, mid_ref
):
    me = me_ref[0]

    def forward(g, carry):
        rows = pl.ds(pl.multiple_of(g * 8, 8), 8)
        rows_im = pl.ds(pl.multiple_of(g * 8 + 32, 8), 8)

        def load(i):
            return in_ref[i, rows, :].astype(F32), in_ref[i, rows_im, :].astype(F32)

        def store(p, value):
            re, im = value
            c, s = tc_ref[p : p + 1, :], ts_ref[p : p + 1, :]
            mid_ref[p, rows, 0:128] = re * c - im * s
            mid_ref[p, rows, 128:256] = re * s + im * c

        major_dft(load, store, scr_ref, 8, 16, -1)
        return carry

    lax.fori_loop(0, 4, forward, 0)

    sub = lax.broadcasted_iota(jnp.int32, (32, 128), 0)
    lane = lax.broadcasted_iota(jnp.int32, (32, 128), 1)
    line = lax.broadcasted_iota(jnp.int32, (1, 128), 1)
    v = me // 2 + 64 * (64 * (me % 2) + 32 * (lane // 64) + sub)
    fx = jnp.where(v < N // 2, v, v - N).astype(F32) * (1.0 / N)
    fx2 = fx * fx
    twice = 2.0 * fx

    def mix(g, carry):
        p0 = g * 8
        lhs = mid_ref[pl.ds(p0, 8), :, :].reshape(256, 256)
        spec = dot3(lhs, fh_ref[...], fl_ref[...])
        parts = []
        for k in range(8):
            re, im = spec[32 * k : 32 * k + 32, 0:128], spec[32 * k : 32 * k + 32, 128:256]
            u = p0 + k + 128 * (line % 64)
            fy = jnp.where(u < N // 2, u, u - N).astype(F32) * (1.0 / N)
            fy2 = fy * fy
            q = fx2 + fy2
            inv = 1.0 / jnp.where(q > 0, q, 1.0)
            kr = (fx2 - fy2) * inv
            ki = twice * fy * inv
            parts.append(jnp.concatenate([kr * re + ki * im, kr * im - ki * re], 1))
        hat = jnp.concatenate(parts, 0)
        back = dot3(hat, gh_ref[...], gl_ref[...])
        for k in range(8):
            re, im = back[32 * k : 32 * k + 32, 0:128], back[32 * k : 32 * k + 32, 128:256]
            c, s = tc_ref[pl.ds(p0 + k, 1), :], ts_ref[pl.ds(p0 + k, 1), :]
            mid_ref[p0 + k, :, 0:128] = (re * c + im * s) * (1.0 / N)
            mid_ref[p0 + k, :, 128:256] = (im * c - re * s) * (1.0 / N)
        return carry

    lax.fori_loop(0, 16, mix, 0, unroll=16)

    def inverse(g, carry):
        rows = pl.ds(pl.multiple_of(g * 8, 8), 8)
        rows_im = pl.ds(pl.multiple_of(g * 8 + 32, 8), 8)

        def load(i):
            return mid_ref[i, rows, 0:128], mid_ref[i, rows, 128:256]

        def store(a, value):
            re, im = value
            out_ref[a, rows, :] = re.astype(BF16)
            out_ref[a, rows_im, :] = im.astype(BF16)

        major_dft(load, store, scr_ref, 8, 16, 1)
        return carry

    lax.fori_loop(0, 4, inverse, 0)


def back_kernel(
    in_ref, tc_ref, ts_ref, wh_ref, wl_ref, e_hbm, b_hbm, scr_ref, mid_ref, e_ref, b_ref, sems
):
    def leave(g, which):
        rows = pl.ds(pl.multiple_of(g * 8, 8), 8)
        source, target = ((e_ref, e_hbm), (b_ref, b_hbm))[which]
        return pltpu.make_async_copy(source.at[rows], target.at[rows], sems.at[g, which])

    def mix(g, carry):
        p = g * 4
        pieces = []
        for k in range(4):
            part = in_ref[pl.ds(2 * (p + k), 2), :, :].reshape(128, 128).astype(F32).T
            pieces.append(jnp.concatenate([part[0:64], part[64:128]], 1))
        lhs = jnp.concatenate(pieces, 0).astype(BF16)
        out = dot(lhs, wh_ref[...]) + dot(lhs, wl_ref[...])
        for k in range(4):
            re, im = out[64 * k : 64 * k + 64, 0:128], out[64 * k : 64 * k + 64, 128:256]
            c, s = tc_ref[pl.ds(p + k, 1), :], ts_ref[pl.ds(p + k, 1), :]
            mid_ref[p + k, :, 0:128] = re * c - im * s
            mid_ref[p + k, :, 128:256] = re * s + im * c
        return carry

    lax.fori_loop(0, 16, mix, 0, unroll=16)

    def row_group(g, carry):
        rows = pl.ds(pl.multiple_of(g * 8, 8), 8)

        def load(i):
            return mid_ref[i, rows, 0:128], mid_ref[i, rows, 128:256]

        def store(a, value):
            e_ref[rows, a * 128 : a * 128 + 128] = value[0]
            b_ref[rows, a * 128 : a * 128 + 128] = value[1]

        major_dft(load, store, scr_ref, 8, 8, 1)
        leave(g, 0).start()
        leave(g, 1).start()
        return carry

    lax.fori_loop(0, 8, row_group, 0)
    for g in range(8):
        leave(g, 0).wait()
        leave(g, 1).wait()


def exchange(x):
    return lax.all_to_all(x, ("blk", "col"), split_axis=0, concat_axis=0, tiled=True)


def on_chip(x):
    return pltpu.with_memory_space_constraint(x, pltpu.VMEM)


def pack_call(*args):
    return pl.pallas_call(
        pack_kernel,
        out_shape=pltpu.VMEM((128, 2, 1280), BF16),
        in_specs=[HBM] * 6,
        out_specs=VMEM,
        scratch_shapes=[
            pltpu.VMEM((1, 256), jnp.int32),
            pltpu.VMEM((2, 256, 256), jnp.int32),
            pltpu.VMEM((3, 256, 256), F32),
            pltpu.SemaphoreType.DMA((6,)),
        ],
        compiler_params=pltpu.CompilerParams(vmem_limit_bytes=LIMIT),
        name="pack",
    )(*(pltpu.with_memory_space_constraint(x, pltpu.HBM) for x in args))


def row_call(got):
    tags = got[:, 768].astype(F32)
    high = got[:, 1024].astype(F32)
    a = (jnp.abs(tags) - 1.0).astype(jnp.int32)
    band = a // 32
    tile = jnp.arange(256, dtype=jnp.int32) // 2 % 4
    block = tile * 16 + a % 4 + jnp.where(high >= 128.0, 4, 0) + jnp.where(tags < 0, 8, 0)
    tc, ts = twiddle_table(64, np.arange(128), -1, 1.0)
    wh, wl = split_table(row_table())
    return pl.pallas_call(
        row_kernel,
        out_shape=pltpu.VMEM((DEV, 64, 128), BF16),
        in_specs=[SMEM, SMEM] + [VMEM] * 5,
        out_specs=VMEM,
        scratch_shapes=[
            pltpu.VMEM((3, 64, 64, 128), F32),
            pltpu.VMEM((2, 64, 8, 128), F32),
            pltpu.VMEM((64, 64, 256), F32),
        ],
        compiler_params=pltpu.CompilerParams(vmem_limit_bytes=LIMIT),
        name="rows",
    )(band, block, got, tc, ts, wh, wl)


def col_call(me, x):
    tc, ts = twiddle_table(128, np.arange(128) % 64, -1, 1.0)
    fh, fl = split_table(col_table(-1))
    gh, gl = split_table(col_table(1))
    return pl.pallas_call(
        col_kernel,
        out_shape=pltpu.VMEM((DEV, 64, 128), BF16),
        in_specs=[SMEM] + [VMEM] * 7,
        out_specs=VMEM,
        scratch_shapes=[pltpu.VMEM((2, 128, 8, 128), F32), pltpu.VMEM((128, 32, 256), F32)],
        compiler_params=pltpu.CompilerParams(vmem_limit_bytes=LIMIT),
        name="columns",
    )(me, x, tc, ts, fh, fl, gh, gl)


def back_call(x):
    tc, ts = twiddle_table(64, np.arange(128), 1, 1.0 / N)
    wh, wl = split_table(row_inverse_table())
    return pl.pallas_call(
        back_kernel,
        out_shape=(jax.ShapeDtypeStruct((64, N), F32), jax.ShapeDtypeStruct((64, N), F32)),
        in_specs=[VMEM] * 5,
        out_specs=(HBM, HBM),
        scratch_shapes=[
            pltpu.VMEM((2, 64, 8, 128), F32),
            pltpu.VMEM((64, 64, 256), F32),
            pltpu.VMEM((64, N), F32),
            pltpu.VMEM((64, N), F32),
            pltpu.SemaphoreType.DMA((8, 2)),
        ],
        compiler_params=pltpu.CompilerParams(vmem_limit_bytes=LIMIT),
        name="back",
    )(x, tc, ts, wh, wl)


def local(pixel_row, pixel_col, strip_of_span, shear_one, shear_two, weight):
    me = (lax.axis_index("blk") * lax.axis_size("col") + lax.axis_index("col")).reshape(1)
    me, pixel_row = lax.optimization_barrier((me.astype(jnp.int32), pixel_row))
    sent = pack_call(pixel_row, pixel_col, strip_of_span, shear_one, shear_two, weight)
    got = exchange(sent).reshape(256, 1280)
    columns = exchange(row_call(got))
    rows = exchange(col_call(me, on_chip(columns)))
    return back_call(on_chip(rows))


def solution(mesh):
    placed = (P(("blk", "col"), None),) * 6
    return jax.shard_map(
        local,
        mesh=mesh,
        in_specs=placed,
        out_specs=(P(("blk", "col"), None), P(("blk", "col"), None)),
        check_vma=False,
    )
```
